32 devices in a mesh: dp: 16 (over z, x, core), cls: 2 (over y).
Axes of the slice: x: 2, y: 2, z: 4, core: 2. Of those that a mesh axis runs over, the one named last changes fastest.
Arguments:
- features: bfloat16 [512, 65536], P('cls', 'dp'), may hold values from -200 to 200
- labels: int32 [65536], P('dp'), may hold values from 0 to 7
- coeffs: bfloat16 [8, 512], P('cls'), may hold values from -0.176776695 to 0.176776695
- smoothing: float32 [8], replicated, may hold values from 0.1 to 1
- pair_slots: int32 [36], P('cls'), may hold values from 0 to 35, each once
Outputs:
- hessian: float32 [512, 36, 512], P('dp', 'cls')
- gradient: float32 [8, 512], P('cls', 'dp')
The draws below stay inside these ranges and needn't reach their ends.
Inputs may be any that keep to these rules, and one draw needn't show every extreme that they name: `pair_slots`: the entry of slot s of the index c of cls is entry c * 18 + s; an entry below 36 names that pair block, a larger entry marks an empty slot; every value appears once.
All inputs are finite; a program needn't handle non-finite values.
Results may differ from the reference program's by a relative error of at most 0.0003.
Values may be sent and summed in bfloat16 or wider, within the bound.
A program may use at most 256 MiB of HBM per device.

```python
import math
import jax
import jax.numpy as jnp
import numpy as np
from jax import lax

CLASSES = 8
BASIS = 512
ROWS_DEV = 4096
ROWS = 65536
PAIRS = 36
SLOTS = 18
N_CLS = 2


def coeff_table(key):
    values = jax.random.truncated_normal(jax.random.fold_in(key, 11), -4.0, 4.0, (CLASSES, BASIS), jnp.float32)
    return values / math.sqrt(BASIS)


def draw_coeffs(key, part):
    return coeff_table(key).astype(jnp.bfloat16)


def draw_features(key, part):
    values = jax.random.truncated_normal(jax.random.fold_in(key, 12), -6.0, 6.0, (ROWS, BASIS), jnp.float32)
    return jnp.clip(values, -200.0, 200.0).T.astype(jnp.bfloat16)


def place_ends(entries, key, low, top_value):
    spot = [jax.random.randint(jax.random.fold_in(key, axis), (), 0, length) for axis, length in enumerate(entries.shape)]
    widest = entries.shape.index(max(entries.shape))
    beside = spot[:widest] + [(spot[widest] + 1) % entries.shape[widest]] + spot[widest + 1:]
    return entries.at[tuple(spot)].set(low).at[tuple(beside)].set(top_value)


def setup_inputs(seed: int = 0) -> dict:
    seeds = jax.random.split(jax.random.key(seed), 6)
    features = draw_features(jax.random.fold_in(seeds[5], 71), 0)
    labels = place_ends(jax.random.randint(seeds[1], (ROWS,), 0, CLASSES), jax.random.fold_in(seeds[1], 1), 0, CLASSES - 1).astype(jnp.int32)
    coeffs = draw_coeffs(jax.random.fold_in(seeds[5], 71), 0)
    smoothing = jnp.clip(jnp.exp(jax.random.uniform(seeds[3], (CLASSES,), jnp.float32, math.log(0.1), math.log(1.0))), 0.1, 1.0)
    pair_slots = jax.random.permutation(seeds[4], N_CLS * SLOTS).astype(jnp.int32)
    return dict(features=features, labels=labels, coeffs=coeffs, smoothing=smoothing, pair_slots=pair_slots)


def pair_tables():
    first_list = []
    second_list = []
    for class_one in range(CLASSES):
        for class_two in range(class_one, CLASSES):
            first_list.append(class_one)
            second_list.append(class_two)
    return np.array(first_list, np.int32), np.array(second_list, np.int32)


def second_differences(width):
    index_row = jnp.arange(width - 2)[:, None]
    index_col = jnp.arange(width)[None, :]
    return ((index_col == index_row).astype(jnp.float32) - 2.0 * (index_col == index_row + 1).astype(jnp.float32)
            + (index_col == index_row + 2).astype(jnp.float32))


def reference(features, labels, coeffs, smoothing, pair_slots):
    matrix = features.T
    scores = jnp.dot(matrix, coeffs.T, preferred_element_type=jnp.float32)
    row_top = jnp.max(scores, axis=1, keepdims=True)
    exponent = jnp.exp(scores - row_top)
    probs = exponent / jnp.sum(exponent, axis=1, keepdims=True)
    differences = second_differences(BASIS)
    penalty_matrix = jnp.dot(differences.T, differences, precision=lax.Precision.HIGHEST,
                             preferred_element_type=jnp.float32)
    first_tab, second_tab = pair_tables()
    first_tab = jnp.asarray(first_tab)
    second_tab = jnp.asarray(second_tab)
    row_weight = 1.0 / ROWS_DEV

    def pair_block(pair_number):
        class_one = first_tab[pair_number]
        class_two = second_tab[pair_number]
        same_class = (class_one == class_two).astype(jnp.float32)
        prob_one = jnp.take(probs, class_one, axis=1)
        prob_two = jnp.take(probs, class_two, axis=1)
        weights = prob_one * (same_class - prob_two)
        scaled = (matrix * weights[:, None]).astype(jnp.bfloat16)
        products = jnp.dot(scaled.T, matrix, preferred_element_type=jnp.float32) * row_weight
        return products + same_class * smoothing[class_one] * penalty_matrix

    blocks = lax.map(pair_block, jnp.arange(PAIRS, dtype=jnp.int32))
    live_slot = (pair_slots < PAIRS).astype(jnp.float32)
    pair_index = jnp.minimum(pair_slots, PAIRS - 1).astype(jnp.int32)
    chosen = blocks[pair_index] * live_slot[:, None, None]
    hessian = jnp.transpose(chosen, (1, 0, 2))
    one_hot = (labels[:, None] == jnp.arange(CLASSES, dtype=jnp.int32)[None, :]).astype(jnp.float32)
    resid = (one_hot - probs).astype(jnp.bfloat16)
    data_part = jnp.dot(resid.T, matrix, preferred_element_type=jnp.float32) * row_weight
    penalty_part = jnp.dot(coeffs.astype(jnp.float32), penalty_matrix, precision=lax.Precision.HIGHEST,
                           preferred_element_type=jnp.float32)
    gradient = data_part - smoothing[:, None] * penalty_part
    return hessian, gradient
```

```python
import jax
import jax.numpy as jnp
from jax import lax
from jax.sharding import PartitionSpec as P

CLASSES = 8


def pair_tables():
    first_list = []
    second_list = []
    for class_one in range(CLASSES):
        for class_two in range(class_one, CLASSES):
            first_list.append(class_one)
            second_list.append(class_two)
    return (jnp.array(first_list, jnp.int32), jnp.array(second_list, jnp.int32))


def second_differences(width):
    index_row = jnp.arange(width - 2)[:, None]
    index_col = jnp.arange(width)[None, :]
    return (
        (index_col == index_row).astype(jnp.float32)
        - 2.0 * (index_col == index_row + 1).astype(jnp.float32)
        + (index_col == index_row + 2).astype(jnp.float32)
    )


SLOT_GROUP = 3


def exchange_rows(features):
    parts = lax.axis_size("cls")
    if parts != 2:
        return lax.all_gather(features, "cls", axis=0, tiled=True)
    other = lax.ppermute(features, "cls", [(0, 1), (1, 0)])
    is_low = lax.axis_index("cls") == 0
    low = jnp.where(is_low, features, other)
    high = jnp.where(is_low, other, features)
    return jnp.concatenate([low, high], axis=0)


def halves(array, axis, mine):
    zero = lax.index_in_dim(array, 0, axis, False)
    one = lax.index_in_dim(array, 1, axis, False)
    stays_low = mine == 0
    return jnp.where(stays_low, zero, one), jnp.where(stays_low, one, zero)


class GroupSum:
    def __init__(self, blocks, swap):
        self.owners = lax.axis_size("dp")
        self.bits = self.owners.bit_length() - 1
        self.share = blocks[0].shape[0] // self.owners
        self.order = list(range(self.bits))
        if swap and self.bits > 2:
            self.order[1], self.order[2] = self.order[2], self.order[1]
        self.left = list(range(self.bits - 1, -1, -1))
        self.blocks = blocks
        self.held = None
        self.kept = None
        self.moving = None

    def launch(self):
        if not self.order:
            return
        bit = self.order.pop(0)
        axis = self.left.index(bit)
        self.left.remove(bit)
        mine = (lax.axis_index("dp") >> bit) & 1
        if self.held is None:
            shape = (2,) * self.bits + (self.share, self.blocks[0].shape[1])
            parts = [halves(block.reshape(shape), axis, mine) for block in self.blocks]
            self.kept = jnp.stack([part[0] for part in parts], axis=0)
            sent = jnp.stack([part[1] for part in parts], axis=0)
        else:
            self.kept, sent = halves(self.held, axis + 1, mine)
        pairs = [(owner, owner ^ (1 << bit)) for owner in range(self.owners)]
        self.moving = lax.ppermute(sent, "dp", pairs)

    def land(self):
        if self.moving is None:
            return
        self.held = self.kept + self.moving
        self.moving = None
        self.launch()

    def finish(self):
        if self.owners != 1 << self.bits:
            stacked = jnp.stack(self.blocks, axis=0)
            return lax.psum_scatter(stacked, "dp", scatter_dimension=1, tiled=True)
        while self.moving is not None:
            self.land()
        return self.held


def local(features, labels, coeffs, smoothing, pair_slots):
    row_count = features.shape[1]
    own_width = features.shape[0]
    width = own_width * lax.axis_size("cls")
    row_share = width // lax.axis_size("dp")
    local_classes = coeffs.shape[0]
    slot_count = pair_slots.shape[0]
    row_weight = 1.0 / row_count
    cls_index = lax.axis_index("cls")
    gathered = exchange_rows(features)
    every_coeff = lax.all_gather(coeffs, "cls", axis=0, tiled=True)
    own_coeff = lax.dynamic_slice_in_dim(every_coeff, cls_index * own_width, own_width, 1)
    scores = lax.psum(
        jnp.dot(own_coeff, features, preferred_element_type=jnp.float32), "cls"
    )
    exponent = jnp.exp(scores - jnp.max(scores, axis=0)[None, :])
    every_prob = exponent / jnp.sum(exponent, axis=0)[None, :]
    class_start = cls_index * local_classes
    probs = lax.dynamic_slice_in_dim(every_prob, class_start, local_classes, 0)
    own_classes = class_start + jnp.arange(local_classes, dtype=jnp.int32)
    one_hot = (labels[None, :] == own_classes[:, None]).astype(jnp.float32)
    resid = (one_hot - probs).astype(jnp.bfloat16)
    grad_term = (
        lax.dot_general(
            resid, gathered, (((1,), (1,)), ((), ())), preferred_element_type=jnp.float32
        )
        * row_weight
    )
    grad_share = lax.psum_scatter(grad_term, "dp", scatter_dimension=1, tiled=True)
    row_start = lax.axis_index("dp") * row_share
    differences = second_differences(width)
    own_columns = lax.dynamic_slice_in_dim(differences, row_start, row_share, 1)
    penalty_rows = jnp.dot(
        own_columns.T,
        differences,
        precision=lax.Precision.HIGHEST,
        preferred_element_type=jnp.float32,
    )
    own_smoothing = lax.dynamic_slice_in_dim(smoothing, class_start, local_classes, 0)
    penalty_part = jnp.dot(
        coeffs.astype(jnp.float32),
        penalty_rows.T,
        precision=lax.Precision.HIGHEST,
        preferred_element_type=jnp.float32,
    )
    gradient = grad_share - own_smoothing[:, None] * penalty_part
    first_tab, second_tab = pair_tables()
    pair_count = first_tab.shape[0]
    live_slot = (pair_slots < pair_count).astype(jnp.float32)
    pair_index = jnp.minimum(pair_slots, pair_count - 1)
    pick_pair = pair_index[:, None] == jnp.arange(pair_count, dtype=jnp.int32)[None, :]
    first_class = jnp.sum(jnp.where(pick_pair, first_tab[None, :], 0), axis=1)
    second_class = jnp.sum(jnp.where(pick_pair, second_tab[None, :], 0), axis=1)
    class_range = jnp.arange(CLASSES, dtype=jnp.int32)[None, :]
    select_first = (first_class[:, None] == class_range).astype(jnp.float32)
    select_second = (second_class[:, None] == class_range).astype(jnp.float32)
    prob_first = jnp.dot(
        select_first,
        every_prob,
        precision=lax.Precision.HIGHEST,
        preferred_element_type=jnp.float32,
    )
    prob_second = jnp.dot(
        select_second,
        every_prob,
        precision=lax.Precision.HIGHEST,
        preferred_element_type=jnp.float32,
    )
    same_class = (first_class == second_class).astype(jnp.float32)
    weights = live_slot[:, None] * (prob_first * (same_class[:, None] - prob_second))
    groups = []
    power_of_two = lax.axis_size("dp") & (lax.axis_size("dp") - 1) == 0
    for number, start in enumerate(range(0, slot_count, SLOT_GROUP)):
        if power_of_two:
            for back in (5, 2):
                if number >= back:
                    earlier = groups[number - back]
                    earlier.land()
                    weights, earlier.held, earlier.kept = lax.optimization_barrier(
                        (weights, earlier.held, earlier.kept)
                    )
        blocks = []
        for slot in range(start, min(start + SLOT_GROUP, slot_count)):
            scaled = (gathered * weights[slot][None, :]).astype(jnp.bfloat16)
            blocks.append(
                lax.dot_general(
                    scaled,
                    gathered,
                    (((1,), (1,)), ((), ())),
                    preferred_element_type=jnp.float32,
                )
            )
        groups.append(GroupSum(blocks, number % 2 == 1))
        if power_of_two:
            groups[-1].launch()
    sums = [group.finish() for group in groups]
    own_rows = jnp.transpose(jnp.concatenate(sums, axis=0), (1, 0, 2)) * row_weight
    slot_smoothing = jnp.dot(
        select_first, smoothing, precision=lax.Precision.HIGHEST, preferred_element_type=jnp.float32
    )
    penalty = live_slot * same_class * slot_smoothing
    hessian = (
        own_rows
        + penalty[None, :, None] * penalty_rows[:, None, :]
    )
    return (hessian, gradient)


def solution(mesh):
    return jax.shard_map(
        local,
        mesh=mesh,
        in_specs=(P("cls", "dp"), P("dp"), P("cls", None), P(), P("cls")),
        out_specs=(P("dp", "cls", None), P("cls", "dp")),
        check_vma=False,
    )
```
